32 devices in a mesh: row: 2 (over y), col: 16 (over z, x, core).
Axes of the slice: x: 2, y: 2, z: 4, core: 2. Of those that a mesh axis runs over, the one named last changes fastest.
Arguments:
- pair_grad: float32 [1024, 1024, 128], P('row', 'col'), may hold values from -4 to 4
- out_weight: bfloat16 [1024, 128], replicated, may hold values from -0.1875 to 0.1875
- left_factor: bfloat16 [32, 32, 1024], P('col', None, 'row'), may hold values from -6 to 6
- right_factor: bfloat16 [32, 32, 1024], P('row', None, 'col'), may hold values from -6 to 6
Outputs:
- left_grad: float32 [32, 32, 1024], P('col', None, 'row')
- right_grad: float32 [32, 32, 1024], P('row', None, 'col')
The draws below stay inside these ranges and needn't reach their ends.
All inputs are finite; a program needn't handle non-finite values.
Results may differ from the reference program's by a relative error of at most 0.0042.
Values may be sent and summed in bfloat16 or wider, within the bound.
No kernel may reach another device: no remote copies, remote signals or barrier semaphores. Data moves between devices by JAX's collectives and lax.ppermute only.
A program may use at most 192 MiB of HBM per device.

```python
import math
import jax
import jax.numpy as jnp
from jax import lax

C = 32
P_SIZE = 128
S = 32
TOKENS = 1024


def levels(rng, dims, split, smallest, top_value):
    def one(position, parts):
        draws = jax.random.uniform(jax.random.fold_in(jax.random.fold_in(rng, 6), position), (parts,), jnp.float32, smallest / len(split), top_value / len(split))
        return jnp.repeat(jnp.exp(draws), dims[position] // parts).reshape((-1,) + (1,) * (len(dims) - position - 1))

    factor_of = one(*split[0])
    for cut in split[1:]:
        factor_of = factor_of * one(*cut)
    return factor_of


def noise(key, dims, deviation, reach, pieces=(), kind=jnp.bfloat16):
    loudness = levels(key, dims, pieces, -0.22, 0.18) if pieces else 1.0
    array = jax.random.normal(key, dims, jnp.float32) * deviation * loudness
    return jnp.minimum(jnp.maximum(array, -reach), reach).astype(kind)


def setup_inputs(seed: int = 0) -> dict:
    seeds = jax.random.split(jax.random.key(seed), 5)
    pair_grad = noise(seeds[0], (TOKENS, TOKENS, P_SIZE), 0.5, 4.0, ((0, 2), (1, 16)), jnp.float32)
    out_weight = noise(seeds[1], (C * C, P_SIZE), (C * C) ** -0.5, 0.1875)
    left_factor = noise(seeds[2], (S, C, TOKENS), 1.0, 6.0, ((0, 16), (2, 2)))
    right_factor = noise(seeds[3], (S, C, TOKENS), 1.0, 6.0, ((0, 2), (2, 16)))
    return dict(pair_grad=pair_grad, out_weight=out_weight, left_factor=left_factor, right_factor=right_factor)


def reference(pair_grad, out_weight, left_factor, right_factor):
    rows_per_block = math.gcd(TOKENS, 32)
    sequence_count = TOKENS // rows_per_block
    pair_low = pair_grad.astype(jnp.bfloat16)
    grid = out_weight.astype(jnp.float32).reshape(C, C, P_SIZE)
    left_wide = left_factor.astype(jnp.float32)
    right_wide = right_factor.astype(jnp.float32)

    def step(carry, index):
        start = (index * rows_per_block).astype(jnp.int32)
        block = lax.dynamic_slice_in_dim(pair_low, start, rows_per_block, 0).astype(jnp.float32)
        expanded = jnp.einsum("ijk,xyk->ijxy", block, grid).astype(jnp.bfloat16)
        expanded = lax.optimization_barrier(expanded).astype(jnp.float32)
        left_block = lax.dynamic_slice_in_dim(left_wide, start, rows_per_block, 2)
        left_portion = jnp.einsum("ijxy,syj->sxi", expanded, right_wide)
        carry = carry + jnp.einsum("ijxy,sxi->syj", expanded, left_block)
        return carry, left_portion

    initial_carry = jnp.zeros((S, C, TOKENS), jnp.float32)
    right_total, left_portions = lax.scan(step, initial_carry, jnp.arange(sequence_count, dtype=jnp.int32))
    left_total = jnp.transpose(left_portions, (1, 2, 0, 3)).reshape(S, C, TOKENS)
    return left_total * (1.0 / S), right_total * (1.0 / S)
```

```python
import functools

import jax
import jax.numpy as jnp
from jax import lax
from jax.experimental import pallas as pl
from jax.experimental.pallas import tpu as pltpu
from jax.sharding import PartitionSpec as P

F32 = jnp.float32
BF16 = jnp.bfloat16
NT = (((1,), (1,)), ((), ()))
LANES = 128
TILE = 16


def stage_masks(ncol):
    bits = ncol.bit_length() - 1
    return [1, 2] + [1 << b for b in range(bits - 1, 1, -1)]


def bit(value, mask):
    return lax.shift_right_logical(value, mask.bit_length() - 1) & 1


def left_kernel(first, last, has_prev, scale, offsets, masks, per, *refs):
    n = len(offsets)
    pair_ref, w_ref = refs[0], refs[1]
    r_refs = refs[2:2 + n]
    rest = list(refs[2 + n:])
    prev_ref = rest.pop(0) if has_prev else None
    pb_ref = rest.pop(0) if first else None
    out_refs = [rest.pop(0) for _ in range(2 if last else 1)]
    rt_ref, a_ref, acc_ref = rest[:3]
    buf_ref = rest[3] if last else out_refs[0]
    srow, ydim, jdim = r_refs[0].shape
    rows = n * srow
    kdim = w_ref.shape[1]
    xdim = w_ref.shape[0] // ydim
    bj = a_ref.shape[1] // kdim
    nb = acc_ref.shape[0]
    g = pl.program_id(0)

    @pl.when(g == 0)
    def _():
        for d in range(n):
            for t in range(srow):
                v = jnp.concatenate([r_refs[d][t].astype(F32), jnp.zeros((LANES - ydim, jdim), F32)], axis=0)
                rt_ref[pl.ds(d * srow + t, jdim, stride=rows), :] = v.T
        acc_ref[...] = jnp.zeros_like(acc_ref)

    start = pl.multiple_of(g * (bj * rows), bj * rows)
    lhs = rt_ref[pl.ds(start, bj * rows), :][:, :ydim].astype(BF16)
    for x in range(0, xdim, 2):
        wx = jnp.concatenate([w_ref[(x + h) * ydim:(x + h + 1) * ydim, :] for h in range(2)], axis=1)
        zz = jnp.dot(lhs, wx, preferred_element_type=F32).astype(BF16)
        for h in range(2):
            for j in range(bj):
                a_ref[(x + h) * rows:(x + h + 1) * rows, j * kdim:(j + 1) * kdim] = (
                    zz[j * rows:(j + 1) * rows, h * kdim:(h + 1) * kdim])
    if first:
        idim = pair_ref.shape[0]
        flat = pair_ref.reshape(idim * bj, kdim)
        for j in range(bj):
            pb_ref[0, :, j * kdim:(j + 1) * kdim] = flat[pl.ds(j, idim, stride=bj), :].astype(BF16)
        rhs = pb_ref[0]
    else:
        rhs = pair_ref[0]
    part = lax.dot_general(a_ref[...], rhs, NT, preferred_element_type=F32)
    for b in range(nb):
        acc_ref[b] += part[:, b * LANES:(b + 1) * LANES]

    @pl.when(g == pl.num_programs(0) - 1)
    def _():
        row_at = lax.axis_index("row")
        col_at = lax.axis_index("col")
        if has_prev:
            buf_ref[...] = prev_ref[...]
        for d in range(n):
            for t in range(srow):
                whole_row = (row_at ^ offsets[d]) * srow + t
                rel = lax.div(whole_row, per) ^ col_at
                slot = sum(bit(rel, m) << (len(masks) - 1 - k) for k, m in enumerate(masks))
                inner = lax.rem(whole_row, per)
                for b in range(nb):
                    v = acc_ref[b, pl.ds(d * srow + t, xdim, stride=rows), :] * scale
                    buf_ref[slot, inner, :, b * LANES:(b + 1) * LANES] = v.astype(BF16)
        if last:
            half = buf_ref.shape[0] // 2
            out_refs[0][...] = buf_ref[:half]
            out_refs[1][...] = buf_ref[half:]


def right_kernel(last, has_prev, scale, rels, nrow, *refs):
    pb_ref, w_ref = refs[0], refs[1]
    l_refs = refs[2:4]
    rest = list(refs[4:])
    prev_ref = rest.pop(0) if has_prev else None
    out_refs = [rest.pop(0) for _ in range(nrow if last else 1)]
    lf_ref, lt_ref, wy_ref, h_ref, o_ref = rest[:5]
    buf_ref = rest[5] if last else out_refs[0]
    n, per, xdim, idim = l_refs[0].shape
    rows = 2 * n * per
    kdim = w_ref.shape[1]
    ydim = w_ref.shape[0] // xdim
    bj = pb_ref.shape[2] // kdim
    jdim = o_ref.shape[0] // rows
    nb = lf_ref.shape[0]
    srow = buf_ref.shape[1]
    g = pl.program_id(0)

    @pl.when(g == 0)
    def _():
        for a in range(2):
            for d in range(n):
                for t in range(per):
                    v = l_refs[a][d, t].astype(F32)
                    for b in range(nb):
                        lf_ref[b, pl.ds((a * n + d) * per + t, xdim, stride=rows), :] = v[:, b * LANES:(b + 1) * LANES]
        for b in range(nb):
            lt_ref[:, b * LANES:(b + 1) * LANES] = lf_ref[b].astype(BF16)
        for x in range(xdim):
            wy_ref[:, x * kdim:(x + 1) * kdim] = w_ref[x * ydim:(x + 1) * ydim, :]

    xs = min(8, xdim)
    for x in range(0, xdim, xs):
        u = jnp.dot(lt_ref[x * rows:(x + xs) * rows, :], pb_ref[0], preferred_element_type=F32).astype(BF16)
        for h in range(xs):
            for j in range(bj):
                h_ref[j * rows:(j + 1) * rows, (x + h) * kdim:(x + h + 1) * kdim] = (
                    u[h * rows:(h + 1) * rows, j * kdim:(j + 1) * kdim])
    res = lax.dot_general(h_ref[...], wy_ref[...], NT, preferred_element_type=F32)
    start = pl.multiple_of(g * (bj * rows), bj * rows)
    o_ref[pl.ds(start, bj * rows), 0:ydim] = res * scale

    @pl.when(g == pl.num_programs(0) - 1)
    def _():
        row_at = lax.axis_index("row")
        col_at = lax.axis_index("col")
        if has_prev:
            buf_ref[...] = prev_ref[...]
        for i, rel in enumerate(rels):
            for t in range(per):
                whole_row = (col_at ^ rel) * per + t
                owner = lax.div(whole_row, srow) ^ row_at
                inner = lax.rem(whole_row, srow)
                buf_ref[owner, inner] = o_ref[pl.ds(i * per + t, jdim, stride=rows), :].T[:ydim]
        if last:
            for q in range(nrow):
                out_refs[q][...] = buf_ref[q].astype(out_refs[q].dtype)


def whole(a):
    zeros = (0,) * len(a.shape)
    return pl.BlockSpec(a.shape, lambda g: zeros)


def call(kernel, name, steps, ins, in_specs, outs, out_specs, scratch, flops):
    return pl.pallas_call(
        kernel,
        out_shape=outs,
        grid=(steps,),
        in_specs=in_specs,
        out_specs=out_specs,
        scratch_shapes=scratch,
        compiler_params=pltpu.CompilerParams(
            dimension_semantics=("arbitrary",), vmem_limit_bytes=56 << 20),
        name=name,
        cost_estimate=pl.CostEstimate(flops=flops, transcendentals=0, bytes_accessed=8 << 20),
    )(*ins)


def left_call(pair, w, rs, offsets, prev, first, last, bj, scale, masks, per, ncol, name):
    srow, ydim, jdim = rs[0].shape
    rows = len(rs) * srow
    kdim = w.shape[1]
    xdim = w.shape[0] // ydim
    idim = pair.shape[0] if first else pair.shape[1]
    block = pl.BlockSpec((1, idim, bj * kdim), lambda g: (g, 0, 0))
    pair_spec = pl.BlockSpec((idim, bj, kdim), lambda g: (0, g, 0)) if first else block
    ins, in_specs = [pair, w, *rs], [pair_spec, whole(w)] + [whole(r) for r in rs]
    if prev is not None:
        ins.append(prev)
        in_specs.append(whole(prev))
    outs, out_specs = [], []
    if first:
        outs.append(jax.ShapeDtypeStruct((jdim // bj, idim, bj * kdim), BF16))
        out_specs.append(block)
    halves = 2 if last else 1
    for _ in range(halves):
        outs.append(jax.ShapeDtypeStruct((ncol // halves, per, xdim, idim), BF16))
        out_specs.append(whole(outs[-1]))
    scratch = [pltpu.VMEM((jdim * rows, LANES), F32),
               pltpu.VMEM((xdim * rows, bj * kdim), BF16),
               pltpu.VMEM((idim // LANES, xdim * rows, LANES), F32)]
    if last:
        scratch.append(pltpu.VMEM((ncol, per, xdim, idim), BF16))
    kernel = functools.partial(left_kernel, first, last, prev is not None, scale, offsets, masks, per)
    return call(kernel, name, jdim // bj, ins, in_specs, outs, out_specs, scratch,
                2 * rows * xdim * idim * jdim * kdim)


def right_call(pb, w, ls, rels, prev, last, scale, nrow, srow, ydim, name):
    n, per, xdim, idim = ls[0].shape
    rows = 2 * n * per
    kdim = w.shape[1]
    steps, _, width = pb.shape
    bj = width // kdim
    jdim = steps * bj
    ins = [pb, w, *ls]
    in_specs = [pl.BlockSpec((1, idim, width), lambda g: (g, 0, 0)), whole(w)] + [whole(a) for a in ls]
    if prev is not None:
        ins.append(prev)
        in_specs.append(whole(prev))
    if last:
        outs = [jax.ShapeDtypeStruct((srow, ydim, jdim), BF16 if q else F32) for q in range(nrow)]
    else:
        outs = [jax.ShapeDtypeStruct((nrow, srow, ydim, jdim), F32)]
    scratch = [pltpu.VMEM((idim // LANES, xdim * rows, LANES), F32),
               pltpu.VMEM((xdim * rows, idim), BF16),
               pltpu.VMEM((ydim, xdim * kdim), BF16),
               pltpu.VMEM((bj * rows, xdim * kdim), BF16),
               pltpu.VMEM((jdim * rows, LANES), F32)]
    if last:
        scratch.append(pltpu.VMEM((nrow, srow, ydim, jdim), F32))
    kernel = functools.partial(right_kernel, last, prev is not None, scale, rels, nrow)
    return call(kernel, name, steps, ins, in_specs, outs, [whole(o) for o in outs], scratch,
                2 * rows * xdim * idim * jdim * kdim)


def body(nrow, ncol, pair_grad, out_weight, left_factor, right_factor):
    per = left_factor.shape[0]
    srow, ydim, jdim = right_factor.shape
    scale = 1.0 / (per * ncol)
    bj = min(16, jdim)
    masks = stage_masks(ncol)

    def swap_col(a, mask):
        return lax.ppermute(a, "col", [(c, c ^ mask) for c in range(ncol)])

    def swap_row(a, mask):
        return lax.ppermute(a, "row", [(r, r ^ mask) for r in range(nrow)])

    def total(arrays, lo, hi):
        acc = arrays[0][lo:hi].astype(F32)
        for a in arrays[1:]:
            acc = acc + a[lo:hi].astype(F32)
        return acc

    rs = [right_factor] + [swap_row(right_factor, d) for d in range(1, nrow)]
    near, rels = left_factor[None], [0]
    for mask in masks[2:]:
        near = jnp.concatenate([near, swap_col(near, mask)], axis=0)
        rels = rels + [e ^ mask for e in rels]

    if srow % TILE == 0 and nrow > 1:
        groups = [[0], list(range(1, nrow))]
    else:
        groups = [list(range(nrow))]
    prev, pair = None, pair_grad
    for k, group in enumerate(groups):
        got = left_call(pair, out_weight, [rs[d] for d in group], group, prev, k == 0, k == len(groups) - 1,
                        bj, scale, masks, per, ncol, f"left{k}")
        if k == 0:
            pair, got = got[0], got[1:]
        prev = got[0]
    kept, sent = got

    parts = [kept, swap_col(sent, 1)]
    near_core = swap_col(near, 1)
    far = swap_col(near, 2)

    size = ncol // 2
    sends = iter(masks[1:])

    def halve():
        nonlocal size
        size //= 2
        parts.append(swap_col(total(parts, size, 2 * size).astype(BF16), next(sends)))

    halve()
    first = right_call(pair, out_weight, [near, near_core], rels + [e ^ 1 for e in rels], None, False,
                       scale, nrow, srow, ydim, "right0")[0]
    far_core = swap_col(far, 1)
    for _ in range(len(masks) - 2):
        halve()
    outs = right_call(pair, out_weight, [far, far_core], [e ^ 2 for e in rels] + [e ^ 3 for e in rels], first, True,
                      scale, nrow, srow, ydim, "right1")
    right_grad = outs[0]
    for q in range(1, nrow):
        right_grad = right_grad + swap_row(outs[q], q).astype(F32)
    left_grad = total(parts, 0, 1)[0]
    return left_grad, right_grad


def solution(mesh):
    placed = (P("row", "col", None), P(), P("col", None, "row"), P("row", None, "col"))
    return jax.shard_map(
        functools.partial(body, mesh.shape["row"], mesh.shape["col"]),
        mesh=mesh,
        in_specs=placed,
        out_specs=(P("col", None, "row"), P("row", None, "col")),
        check_vma=False,
    )
```
